128 devices in a mesh: ep: 8 (over z, core), fsdp: 16 (over y, x).
Axes of the slice: x: 4, y: 4, z: 4, core: 2. Of those that a mesh axis runs over, the one named last changes fastest.
Arguments:
- train_gate: float32 [64, 2048, 1408], P('ep', 'fsdp'), may hold values from -0.1875 to 0.1875
- train_up: float32 [64, 2048, 1408], P('ep', 'fsdp'), may hold values from -0.1875 to 0.1875
- train_down: float32 [64, 1408, 2048], P('ep', None, 'fsdp'), may hold values from -0.21875 to 0.21875
- router_weight: float32 [2048, 64], P('fsdp', 'ep'), may hold values from -0.125 to 0.125
- router_gain: float32 [2048], P('fsdp'), may hold values from 0.25 to 1.75
Outputs:
- ready_gate: bfloat16 [64, 2048, 1408], P('ep', None, 'fsdp')
- ready_up: bfloat16 [64, 2048, 1408], P('ep', None, 'fsdp')
- ready_down: bfloat16 [64, 1408, 2048], P('ep', 'fsdp')
- scale_gate: float32 [64, 1408], P('ep', 'fsdp')
- scale_up: float32 [64, 1408], P('ep', 'fsdp')
- scale_down: float32 [64, 1408], P('ep', 'fsdp')
- serve_router: bfloat16 [2048, 64], replicated
The draws below stay inside these ranges and needn't reach their ends.
All inputs are finite; a program needn't handle non-finite values. Where the reference program divides by a largest or mean magnitude, that divisor is 1e-20 or more.
Results may differ from the reference program's by a relative error of at most 0.012.
Values may be sent and summed in bfloat16 or wider, within the bound.
No kernel may reach another device: no remote copies, remote signals or barrier semaphores. Data moves between devices by JAX's collectives and lax.ppermute only.
A program may use at most 128 MiB of HBM per device.

```python
import jax
import jax.numpy as jnp

EXPERTS = 64
D_MODEL = 2048
D_EXPERT = 1408


def spiked(array, key, source, target, parts, factor):
    owner, partner = [(jnp.arange(array.shape[axis_at]) // (array.shape[axis_at] // parts)).reshape([-1 if axis == axis_at else 1 for axis in range(array.ndim)]) for axis_at in (source, target)]
    chosen = jax.random.permutation(key, parts)[partner]
    strong = (owner == chosen) | (owner == (partner + parts // 2) % parts)
    return jnp.where(strong, factor * array, array)


def block_levels(rng, extent, cuts, smallest, high):
    loudness = 1.0
    for axis_at, shards_of in cuts:
        heights = jax.random.uniform(jax.random.fold_in(jax.random.fold_in(rng, 6), axis_at), (shards_of,), jnp.float32, smallest / len(cuts), high / len(cuts))
        loudness = loudness * jnp.repeat(jnp.exp(heights), extent[axis_at] // shards_of).reshape((-1,) + (1,) * (len(extent) - 1 - axis_at))
    return loudness


def scatter_about(rng, shape, spread, reach, split=(), dtype=jnp.bfloat16):
    drawn = spread * jax.random.normal(rng, shape, jnp.float32)
    if split:
        drawn = drawn * block_levels(rng, shape, split, -0.22, 0.18)
    return jnp.clip(drawn, -reach, reach).astype(dtype)


def bell_draw_with(key, shape, spread, bound, pieces, heavy, dtype=jnp.bfloat16):
    array = spread * jax.random.normal(key, shape, jnp.float32)
    if pieces:
        array = array * block_levels(key, shape, pieces, -0.22, 0.18)
    return jnp.clip(spiked(array, jax.random.fold_in(key, 3), *heavy), -bound, bound).astype(dtype)


def setup_inputs(seed: int = 0) -> dict:
    splits = jax.random.split(jax.random.key(seed), 6)
    train_gate = bell_draw_with(splits[0], (EXPERTS, D_MODEL, D_EXPERT), D_MODEL ** -0.5, 0.1875, ((0, 8), (1, 16)), (1, 2, 16, 2.0), jnp.float32)
    train_up = bell_draw_with(splits[1], (EXPERTS, D_MODEL, D_EXPERT), D_MODEL ** -0.5, 0.1875, ((0, 8), (1, 16)), (1, 2, 16, 2.0), jnp.float32)
    train_down = bell_draw_with(splits[2], (EXPERTS, D_EXPERT, D_MODEL), D_EXPERT ** -0.5, 0.21875, ((0, 8), (2, 16)), (2, 1, 16, 2.0), jnp.float32)
    router_weight = scatter_about(splits[3], (D_MODEL, EXPERTS), D_MODEL ** -0.5, 0.125, ((0, 16), (1, 8)), jnp.float32)
    router_gain = jnp.clip(1.0 + 0.15 * jax.random.normal(splits[4], (D_MODEL,), jnp.float32), 0.25, 1.75)
    return {"train_gate": train_gate, "train_up": train_up, "train_down": train_down, "router_weight": router_weight, "router_gain": router_gain}


def reference(train_gate, train_up, train_down, router_weight, router_gain):
    scale_gate = jnp.sum(jnp.abs(train_gate), axis=1) / D_MODEL
    ready_gate = (train_gate / jnp.expand_dims(scale_gate, 1)).astype(jnp.bfloat16)
    scale_up = jnp.sum(jnp.abs(train_up), axis=1) / D_MODEL
    ready_up = (train_up / jnp.expand_dims(scale_up, 1)).astype(jnp.bfloat16)
    scale_down = jnp.sum(jnp.abs(train_down), axis=2) / D_MODEL
    ready_down = (train_down / jnp.expand_dims(scale_down, 2)).astype(jnp.bfloat16)
    serve_router = (router_weight * router_gain[:, None]).astype(jnp.bfloat16)
    return ready_gate, ready_up, ready_down, scale_gate, scale_up, scale_down, serve_router
```

```python
import jax
import jax.numpy as jnp
from jax import lax
from jax.experimental import pallas as pl
from jax.experimental.pallas import tpu as pltpu
from jax.sharding import PartitionSpec as P

D_MODEL = 2048
PEERS = 16
OWN = 8
COLS = 88
LANES = 128


def pack_down_kernel(down, router, gain, out):
    step = pl.program_id(0)

    @pl.when(step < OWN)
    def _():
        for peer in range(PEERS):
            out[peer] = down[0, COLS * peer : COLS * (peer + 1), :].astype(jnp.bfloat16)

    @pl.when(step == OWN)
    def _():
        served = (router[...] * gain[...]).astype(jnp.bfloat16)
        for peer in range(PEERS):
            out[peer, 0:OWN, :] = served


def pack_down(down, router, gain):
    return pl.pallas_call(
        pack_down_kernel,
        grid=(OWN + 1,),
        in_specs=[
            pl.BlockSpec((1, PEERS * COLS, LANES), lambda e: (jnp.minimum(e, OWN - 1), 0, 0)),
            pl.BlockSpec((OWN, LANES), lambda e: (0, 0)),
            pl.BlockSpec((1, LANES), lambda e: (0, 0)),
        ],
        out_specs=pl.BlockSpec((PEERS, COLS, LANES), lambda e: (0, e, 0)),
        out_shape=jax.ShapeDtypeStruct((PEERS, OWN * COLS + OWN, LANES), jnp.bfloat16),
        name="pack_down",
    )(down, router, gain)


def pack_columns_kernel(gate, up, out):
    for which, ref in enumerate((gate, up)):
        turned = ref[0].astype(jnp.bfloat16).T
        for peer in range(PEERS):
            out[peer, which, 0] = turned[COLS * peer : COLS * (peer + 1), :]


def pack_columns(gate, up):
    block = pl.BlockSpec((1, LANES, PEERS * COLS), lambda e: (e, 0, 0))
    return pl.pallas_call(
        pack_columns_kernel,
        grid=(OWN,),
        in_specs=[block, block],
        out_specs=pl.BlockSpec((PEERS, 2, 1, COLS, LANES), lambda e: (0, 0, e, 0, 0)),
        out_shape=jax.ShapeDtypeStruct((PEERS, 2, OWN, COLS, LANES), jnp.bfloat16),
        name="pack_columns",
    )(gate, up)


def finish(total_of, ready, scales, step):
    total = jnp.zeros((COLS, LANES), jnp.float32)
    for peer in range(PEERS):
        total = total + jnp.abs(total_of(peer).astype(jnp.float32))
    factor = D_MODEL / jnp.sum(total, axis=1, keepdims=True)
    scales[pl.ds(step, 1), :] = jnp.sum(total.T, axis=0, keepdims=True) / D_MODEL
    for peer in range(PEERS):
        ready[0, :, LANES * peer : LANES * (peer + 1)] = (
            total_of(peer).astype(jnp.float32) * factor
        ).astype(jnp.bfloat16)


def finish_down_kernel(got, ready, scales):
    finish(lambda peer: got[peer], ready, scales, pl.program_id(0))


def finish_columns_kernel(got, ready_gate, ready_up, scales_gate, scales_up):
    step = pl.program_id(0)
    finish(lambda peer: got[peer, 0, 0], ready_gate, scales_gate, step)
    finish(lambda peer: got[peer, 1, 0], ready_up, scales_up, step)


READY = jax.ShapeDtypeStruct((OWN, COLS, D_MODEL), jnp.bfloat16)
SCALE = jax.ShapeDtypeStruct((OWN, COLS), jnp.float32)
READY_BLOCK = pl.BlockSpec((1, COLS, D_MODEL), lambda e: (e, 0, 0))
SCALE_BLOCK = pl.BlockSpec((OWN, COLS), lambda e: (0, 0))


def finish_down(got):
    return pl.pallas_call(
        finish_down_kernel,
        grid=(OWN,),
        in_specs=[pl.BlockSpec((PEERS, COLS, LANES), lambda e: (0, e, 0))],
        out_specs=[READY_BLOCK, SCALE_BLOCK],
        out_shape=[READY, SCALE],
        name="finish_down",
    )(got)


def finish_columns(got):
    return pl.pallas_call(
        finish_columns_kernel,
        grid=(OWN,),
        in_specs=[pl.BlockSpec((PEERS, 2, 1, COLS, LANES), lambda e: (0, 0, e, 0, 0))],
        out_specs=[READY_BLOCK, READY_BLOCK, SCALE_BLOCK, SCALE_BLOCK],
        out_shape=[READY, READY, SCALE, SCALE],
        name="finish_columns",
    )(got)


def to_owners(parts):
    return lax.all_to_all(parts, "fsdp", split_axis=0, concat_axis=0, tiled=True)


def shards(train_gate, train_up, train_down, router_weight, router_gain):
    got_down = to_owners(
        pack_down(train_down, jnp.swapaxes(router_weight, 0, 1), router_gain[None, :])
    )
    got_columns = to_owners(pack_columns(train_gate, train_up))
    rows = jnp.swapaxes(got_down[:, OWN * COLS :, :], 0, 1).reshape(OWN, D_MODEL)
    serve_router = lax.all_gather(rows, "ep", axis=0, tiled=True)
    ready_down, scale_down = finish_down(got_down)
    ready_gate, ready_up, scale_gate, scale_up = finish_columns(got_columns)
    return (
        jnp.swapaxes(ready_gate, 1, 2),
        jnp.swapaxes(ready_up, 1, 2),
        ready_down,
        scale_gate,
        scale_up,
        scale_down,
        jnp.swapaxes(serve_router, 0, 1),
    )


def solution(mesh):
    in_specs = (
        P("ep", "fsdp", None),
        P("ep", "fsdp", None),
        P("ep", None, "fsdp"),
        P("fsdp", "ep"),
        P("fsdp"),
    )
    out_specs = (
        P("ep", None, "fsdp"),
        P("ep", None, "fsdp"),
        P("ep", "fsdp", None),
        P("ep", "fsdp"),
        P("ep", "fsdp"),
        P("ep", "fsdp"),
        P(),
    )
    return jax.shard_map(shards, mesh=mesh, in_specs=in_specs, out_specs=out_specs, check_vma=False)
```

```python
import jax
import jax.numpy as jnp
from jax import lax
from jax.experimental import pallas as pl
from jax.experimental.pallas import tpu as pltpu
from jax.sharding import PartitionSpec as P

D_MODEL = 2048
SIDE = 4
PEERS = 16
OWN = 8
COLS = 88
LANES = 128
ROWS = OWN * COLS
FIRST_ROWS = 2 * ROWS + OWN

HOPS = (
    (1, 1), (3, 3),
    (3, 1), (1, 3),
    (0, 2), (2, 0),
    (2, 2),
    (1, 2), (3, 0),
    (3, 2), (1, 0),
    (2, 1), (0, 3),
    (2, 3), (0, 1),
)
HBM = pl.BlockSpec(memory_space=pltpu.HBM)
ANY = pl.BlockSpec(memory_space=pl.ANY)
VMEM = pl.BlockSpec(memory_space=pltpu.VMEM)
SMEM = pl.BlockSpec(memory_space=pltpu.SMEM)


def moved(me, hop, sign):
    y, x = me // SIDE, me % SIDE
    return (y + SIDE + sign * hop[0]) % SIDE * SIDE + (x + SIDE + sign * hop[1]) % SIDE


def started(copies):
    for copy in copies:
        copy.start()
    return copies


def send_out(me, packed, outs, sems):
    copies = started(
        [
            pltpu.make_async_copy(packed.at[moved(me, hop, 1)], out, sems.at[k])
            for k, (hop, out) in enumerate(zip(((0, 0), *HOPS), outs))
        ]
    )
    for copy in copies:
        copy.wait()


def turned_in(raw, packed, base):
    turned = raw[...].astype(jnp.bfloat16).T
    for peer in range(PEERS):
        packed[peer, base : base + COLS, :] = turned[COLS * peer : COLS * (peer + 1), :]


def pack_first_kernel(me, gate, down, router, gain, *rest):
    outs, (raw_gate, raw_down, packed, sems_gate, sems_down, sems_out) = rest[:PEERS], rest[PEERS:]
    gates = [pltpu.make_async_copy(gate.at[e], raw_gate.at[e], sems_gate.at[e]) for e in range(OWN)]
    downs = [pltpu.make_async_copy(down.at[e], raw_down.at[e], sems_down.at[e]) for e in range(OWN)]
    for e in range(OWN):
        gates[e].start()
        downs[e].start()
    served = (router[...] * gain[...]).astype(jnp.bfloat16)
    for peer in range(PEERS):
        packed[peer, 2 * ROWS :, :] = served
    for e in range(OWN):
        gates[e].wait()
        turned_in(raw_gate.at[e], packed, ROWS + COLS * e)
        downs[e].wait()
        for peer in range(PEERS):
            packed[peer, COLS * e : COLS * (e + 1), :] = raw_down[
                e, COLS * peer : COLS * (peer + 1), :
            ].astype(jnp.bfloat16)
    send_out(me[0], packed, outs, sems_out)


def pack_first(me, gate, down, router, gain):
    return pl.pallas_call(
        pack_first_kernel,
        in_specs=[SMEM, HBM, HBM, VMEM, VMEM],
        out_specs=[ANY] * PEERS,
        out_shape=[jax.ShapeDtypeStruct((FIRST_ROWS, LANES), jnp.bfloat16)] * PEERS,
        scratch_shapes=[
            pltpu.VMEM((OWN, LANES, PEERS * COLS), jnp.float32),
            pltpu.VMEM((OWN, PEERS * COLS, LANES), jnp.float32),
            pltpu.VMEM((PEERS, FIRST_ROWS, LANES), jnp.bfloat16),
            pltpu.SemaphoreType.DMA((OWN,)),
            pltpu.SemaphoreType.DMA((OWN,)),
            pltpu.SemaphoreType.DMA((PEERS,)),
        ],
        compiler_params=pltpu.CompilerParams(vmem_limit_bytes=59 << 20),
        name="pack_first",
    )(me, gate, down, router, gain)


def pack_last_kernel(me, up, _, *rest):
    outs, (raw, packed, sems_in, sems_out) = rest[:PEERS], rest[PEERS:]
    copies = started(
        [pltpu.make_async_copy(up.at[e], raw.at[e], sems_in.at[e]) for e in range(OWN)]
    )
    for e in range(OWN):
        copies[e].wait()
        turned_in(raw.at[e], packed, COLS * e)
    send_out(me[0], packed, outs, sems_out)


def pack_last(me, up, after):
    return pl.pallas_call(
        pack_last_kernel,
        in_specs=[SMEM, HBM, ANY],
        out_specs=[ANY] * PEERS,
        out_shape=[jax.ShapeDtypeStruct((ROWS, LANES), jnp.bfloat16)] * PEERS,
        scratch_shapes=[
            pltpu.VMEM((OWN, LANES, PEERS * COLS), jnp.float32),
            pltpu.VMEM((PEERS, ROWS, LANES), jnp.bfloat16),
            pltpu.SemaphoreType.DMA((OWN,)),
            pltpu.SemaphoreType.DMA((PEERS,)),
        ],
        compiler_params=pltpu.CompilerParams(vmem_limit_bytes=10 << 20),
        name="pack_last",
    )(me, up, after)


def finish(got, made, q, e, scales):
    rows = slice(COLS * q, COLS * (q + 1))
    total = jnp.abs(got[0, rows, :].astype(jnp.float32))
    for peer in range(1, PEERS):
        total = total + jnp.abs(got[peer, rows, :].astype(jnp.float32))
    factor = D_MODEL / jnp.sum(total, axis=1, keepdims=True)
    scales[e : e + 1, :] = jnp.sum(total.T, axis=0, keepdims=True) / D_MODEL
    for peer in range(PEERS):
        made[q, :, LANES * peer : LANES * (peer + 1)] = (
            got[peer, rows, :].astype(jnp.float32) * factor
        ).astype(jnp.bfloat16)


def finish_kernel(me, parts, outs, routed, got, made, sems_in, sems_out):
    pair = 2 * COLS
    pairs = len(outs) * OWN // 2
    ranges = [(pair * w, pair) for w in range(pairs)]
    if routed is not None:
        ranges.append((pair * pairs, OWN))
    waves = []
    for wave, (start, size) in enumerate(ranges):
        rows = pl.ds(start, size)
        waves.append(
            started(
                [
                    pltpu.make_async_copy(
                        part.at[rows], got.at[moved(me[0], hop, -1), rows], sems_in.at[wave, k]
                    )
                    for k, (hop, part) in enumerate(zip(((0, 0), *HOPS), parts))
                ]
            )
        )
    writes = []
    for q in range(len(outs) * OWN):
        if q % 2 == 0:
            for copy in waves[q // 2]:
                copy.wait()
        ready, scales = outs[q // OWN]
        finish(got, made, q, q % OWN, scales)
        writes += started(
            [pltpu.make_async_copy(made.at[q], ready.at[q % OWN], sems_out.at[q])]
        )
    if routed is not None:
        for copy in waves[-1]:
            copy.wait()
        for peer in range(PEERS):
            routed[:, LANES * peer : LANES * (peer + 1)] = got[peer, pair * pairs :, :]
    for copy in writes:
        copy.wait()


def finish_first_kernel(me, *rest):
    parts, (down, scale_down, gate, scale_gate, routed, *scratch) = rest[:PEERS], rest[PEERS:]
    got, made, sems_in, sems_out = scratch
    finish_kernel(
        me,
        parts=parts,
        outs=[(down, scale_down), (gate, scale_gate)],
        routed=routed,
        got=got,
        made=made,
        sems_in=sems_in,
        sems_out=sems_out,
    )


def finish_last_kernel(me, _, *rest):
    parts, (up, scale_up, got, made, sems_in, sems_out) = rest[:PEERS], rest[PEERS:]
    finish_kernel(
        me,
        parts=parts,
        outs=[(up, scale_up)],
        routed=None,
        got=got,
        made=made,
        sems_in=sems_in,
        sems_out=sems_out,
    )


READY = jax.ShapeDtypeStruct((OWN, COLS, D_MODEL), jnp.bfloat16)
SCALE = jax.ShapeDtypeStruct((OWN, COLS), jnp.float32)
ROUTED = jax.ShapeDtypeStruct((OWN, D_MODEL), jnp.bfloat16)


def finish_first(me, parts):
    return pl.pallas_call(
        finish_first_kernel,
        in_specs=[SMEM] + [ANY] * PEERS,
        out_specs=[HBM, VMEM, HBM, VMEM, VMEM],
        out_shape=[READY, SCALE, READY, SCALE, ROUTED],
        scratch_shapes=[
            pltpu.VMEM((PEERS, FIRST_ROWS, LANES), jnp.bfloat16),
            pltpu.VMEM((2 * OWN, COLS, D_MODEL), jnp.bfloat16),
            pltpu.SemaphoreType.DMA((OWN + 1, PEERS)),
            pltpu.SemaphoreType.DMA((2 * OWN,)),
        ],
        compiler_params=pltpu.CompilerParams(vmem_limit_bytes=15 << 20),
        name="finish_first",
    )(me, *parts)


def finish_last(me, after, parts):
    return pl.pallas_call(
        finish_last_kernel,
        in_specs=[SMEM, ANY] + [ANY] * PEERS,
        out_specs=[HBM, VMEM],
        out_shape=[READY, SCALE],
        scratch_shapes=[
            pltpu.VMEM((PEERS, ROWS, LANES), jnp.bfloat16),
            pltpu.VMEM((OWN, COLS, D_MODEL), jnp.bfloat16),
            pltpu.SemaphoreType.DMA((OWN // 2, PEERS)),
            pltpu.SemaphoreType.DMA((OWN,)),
        ],
        compiler_params=pltpu.CompilerParams(vmem_limit_bytes=9 << 20),
        name="finish_last",
    )(me, after, *parts)


def to_owners(parts):
    received = [parts[0]]
    for k, hop in enumerate(HOPS):
        route = [(d, moved(d, hop, 1)) for d in range(PEERS)]
        received.append(lax.ppermute(parts[k + 1], "fsdp", route))
    return received


def shards(train_gate, train_up, train_down, router_weight, router_gain):
    me = lax.axis_index("fsdp").astype(jnp.int32)[None]
    router = jnp.swapaxes(router_weight, 0, 1)
    first = pack_first(me, train_gate, train_down, router, router_gain[None, :])
    got_first = to_owners(first)
    last = pack_last(me, train_up, first[0])
    got_last = to_owners(last)
    ready_down, scale_down, ready_gate, scale_gate, routed = finish_first(me, got_first)
    serve_router = lax.all_gather(routed, "ep", axis=0, tiled=True)
    ready_up, scale_up = finish_last(me, serve_router, got_last)
    return (
        jnp.swapaxes(ready_gate, 1, 2),
        jnp.swapaxes(ready_up, 1, 2),
        ready_down,
        scale_gate,
        scale_up,
        scale_down,
        jnp.swapaxes(serve_router, 0, 1),
    )


def solution(mesh):
    in_specs = (
        P("ep", "fsdp", None),
        P("ep", "fsdp", None),
        P("ep", None, "fsdp"),
        P("fsdp", "ep"),
        P("fsdp"),
    )
    out_specs = (
        P("ep", None, "fsdp"),
        P("ep", None, "fsdp"),
        P("ep", "fsdp", None),
        P("ep", "fsdp"),
        P("ep", "fsdp"),
        P("ep", "fsdp"),
        P(),
    )
    return jax.shard_map(shards, mesh=mesh, in_specs=in_specs, out_specs=out_specs, check_vma=False)
```

```python
import jax
import jax.numpy as jnp
from jax import lax
from jax.experimental import pallas as pl
from jax.experimental.pallas import tpu as pltpu
from jax.sharding import PartitionSpec as P

D_MODEL = 2048
SIDE = 4
PEERS = 16
OWN = 8
COLS = 88
LANES = 128
ROWS = OWN * COLS
FIRST_ROWS = 2 * ROWS + OWN
FIRST_LIMIT = 46

HOPS = (
    (1, 1), (3, 3),
    (3, 1), (1, 3),
    (0, 2), (2, 0),
    (2, 2),
    (1, 2), (3, 0),
    (3, 2), (1, 0),
    (2, 1), (0, 3),
    (2, 3), (0, 1),
)
HBM = pl.BlockSpec(memory_space=pltpu.HBM)
ANY = pl.BlockSpec(memory_space=pl.ANY)
VMEM = pl.BlockSpec(memory_space=pltpu.VMEM)
SMEM = pl.BlockSpec(memory_space=pltpu.SMEM)


def moved(me, hop, sign):
    y, x = me // SIDE, me % SIDE
    return (y + SIDE + sign * hop[0]) % SIDE * SIDE + (x + SIDE + sign * hop[1]) % SIDE


def started(copies):
    for copy in copies:
        copy.start()
    return copies


def peers_of(me):
    return [moved(me, hop, 1) for hop in ((0, 0), *HOPS)]


def turned_out(raw, turned, outs, peers, rows):
    whole = raw[...].astype(jnp.bfloat16).T
    for peer in range(PEERS):
        turned[peer] = whole[COLS * peer : COLS * (peer + 1), :]
    for out, peer in zip(outs, peers):
        out[rows, :] = turned[peer]


def cut_out(whole, outs, peers, rows):
    for out, peer in zip(outs, peers):
        part = whole[pl.ds(pl.multiple_of(COLS * peer, 8), COLS), :]
        out[rows, :] = part.astype(jnp.bfloat16)


def pack_first_kernel(me, gate, down, served, *rest):
    outs, (raw_gate, raw_down, turned, sems_gate, sems_down) = rest[:PEERS], rest[PEERS:]
    gates = [pltpu.make_async_copy(gate.at[e], raw_gate.at[e], sems_gate.at[e]) for e in range(OWN)]
    downs = [pltpu.make_async_copy(down.at[e], raw_down.at[e], sems_down.at[e]) for e in range(OWN)]
    for e in range(OWN):
        gates[e].start()
        downs[e].start()
    peers = peers_of(me[0])
    for out in outs:
        out[2 * ROWS :, :] = served[...]
    for e in range(OWN):
        rows = slice(COLS * e, COLS * (e + 1))
        gates[e].wait()
        turned_out(
            raw_gate.at[e], turned.at[e % 2], outs, peers, slice(ROWS + rows.start, ROWS + rows.stop)
        )
        downs[e].wait()
        cut_out(raw_down.at[e], outs, peers, rows)


def pack_first(me, gate, down, served):
    return pl.pallas_call(
        pack_first_kernel,
        in_specs=[SMEM, HBM, HBM, VMEM],
        out_specs=[VMEM] * PEERS,
        out_shape=[jax.ShapeDtypeStruct((FIRST_ROWS, LANES), jnp.bfloat16)] * PEERS,
        scratch_shapes=[
            pltpu.VMEM((OWN, LANES, PEERS * COLS), jnp.float32),
            pltpu.VMEM((OWN, PEERS * COLS, LANES), jnp.float32),
            pltpu.VMEM((2, PEERS, COLS, LANES), jnp.bfloat16),
            pltpu.SemaphoreType.DMA((OWN,)),
            pltpu.SemaphoreType.DMA((OWN,)),
        ],
        compiler_params=pltpu.CompilerParams(vmem_limit_bytes=FIRST_LIMIT << 20),
        name="pack_first",
    )(me, gate, down, served)


def pack_last_kernel(me, up, _, *rest):
    outs, (raw, turned, sems) = rest[:PEERS], rest[PEERS:]
    copies = started([pltpu.make_async_copy(up.at[e], raw.at[e], sems.at[e]) for e in range(OWN)])
    peers = peers_of(me[0])
    for e in range(OWN):
        copies[e].wait()
        turned_out(
            raw.at[e], turned.at[e % 2], outs, peers, slice(COLS * e, COLS * (e + 1))
        )


def pack_last(me, up, after):
    return pl.pallas_call(
        pack_last_kernel,
        in_specs=[SMEM, HBM, ANY],
        out_specs=[VMEM] * PEERS,
        out_shape=[jax.ShapeDtypeStruct((ROWS, LANES), jnp.bfloat16)] * PEERS,
        scratch_shapes=[
            pltpu.VMEM((OWN, LANES, PEERS * COLS), jnp.float32),
            pltpu.VMEM((2, PEERS, COLS, LANES), jnp.bfloat16),
            pltpu.SemaphoreType.DMA((OWN,)),
        ],
        compiler_params=pltpu.CompilerParams(vmem_limit_bytes=10 << 20),
        name="pack_last",
    )(me, up, after)


def factor_of(parts, q, scales):
    rows = slice(COLS * q, COLS * (q + 1))
    total = jnp.abs(parts[0][rows, :].astype(jnp.float32))
    for part in parts[1:]:
        total = total + jnp.abs(part[rows, :].astype(jnp.float32))
    scales[q % OWN : q % OWN + 1, :] = jnp.sum(total.T, axis=0, keepdims=True) / D_MODEL
    return D_MODEL / jnp.sum(total, axis=1, keepdims=True)


def scaled(parts, lanes, made, q, factor):
    rows = slice(COLS * q, COLS * (q + 1))
    for part, here in zip(parts, lanes):
        made[q, :, here] = (part[rows, :].astype(jnp.float32) * factor).astype(jnp.bfloat16)


def finish_kernel(me, parts, outs, routed, made, sems):
    lanes = [
        pl.ds(pl.multiple_of(LANES * moved(me[0], hop, -1), LANES), LANES)
        for hop in ((0, 0), *HOPS)
    ]
    writes = []
    for q in range(len(outs) * OWN):
        ready, scales = outs[q // OWN]
        scaled(parts, lanes, made, q, factor_of(parts, q, scales))
        writes += started([pltpu.make_async_copy(made.at[q], ready.at[q % OWN], sems.at[q])])
    if routed is not None:
        for part, here in zip(parts, lanes):
            routed[:, here] = part[2 * ROWS :, :]
    for copy in writes:
        copy.wait()


def finish_first_kernel(me, *rest):
    parts, (down, scale_down, gate, scale_gate, routed, made, sems) = rest[:PEERS], rest[PEERS:]
    finish_kernel(me, parts, [(down, scale_down), (gate, scale_gate)], routed, made, sems)


def finish_last_kernel(me, _, *rest):
    parts, (up, scale_up, made, sems) = rest[:PEERS], rest[PEERS:]
    finish_kernel(me, parts, [(up, scale_up)], None, made, sems)


READY = jax.ShapeDtypeStruct((OWN, COLS, D_MODEL), jnp.bfloat16)
SCALE = jax.ShapeDtypeStruct((OWN, COLS), jnp.float32)
ROUTED = jax.ShapeDtypeStruct((OWN, D_MODEL), jnp.bfloat16)


def finish_first(me, parts):
    return pl.pallas_call(
        finish_first_kernel,
        in_specs=[SMEM] + [VMEM] * PEERS,
        out_specs=[HBM, VMEM, HBM, VMEM, VMEM],
        out_shape=[READY, SCALE, READY, SCALE, ROUTED],
        scratch_shapes=[
            pltpu.VMEM((2 * OWN, COLS, D_MODEL), jnp.bfloat16),
            pltpu.SemaphoreType.DMA((2 * OWN,)),
        ],
        compiler_params=pltpu.CompilerParams(vmem_limit_bytes=15 << 20),
        name="finish_first",
    )(me, *parts)


def finish_last(me, after, parts):
    return pl.pallas_call(
        finish_last_kernel,
        in_specs=[SMEM, ANY] + [VMEM] * PEERS,
        out_specs=[HBM, VMEM],
        out_shape=[READY, SCALE],
        scratch_shapes=[
            pltpu.VMEM((OWN, COLS, D_MODEL), jnp.bfloat16),
            pltpu.SemaphoreType.DMA((OWN,)),
        ],
        compiler_params=pltpu.CompilerParams(vmem_limit_bytes=9 << 20),
        name="finish_last",
    )(me, after, *parts)


def to_owners(parts):
    received = [parts[0]]
    for k, hop in enumerate(HOPS):
        route = [(d, moved(d, hop, 1)) for d in range(PEERS)]
        received.append(lax.ppermute(parts[k + 1], "fsdp", route))
    return received


def shards(train_gate, train_up, train_down, router_weight, router_gain):
    me = lax.axis_index("fsdp").astype(jnp.int32)[None]
    served = (jnp.swapaxes(router_weight, 0, 1) * router_gain[None, :]).astype(jnp.bfloat16)
    first = pack_first(me, train_gate, train_down, served)
    got_first = to_owners(first)
    last = pack_last(me, train_up, first[0])
    got_last = to_owners(last)
    ready_down, scale_down, ready_gate, scale_gate, routed = finish_first(me, got_first)
    serve_router = lax.all_gather(routed, "ep", axis=0, tiled=True)
    ready_up, scale_up = finish_last(me, serve_router, got_last)
    return (
        jnp.swapaxes(ready_gate, 1, 2),
        jnp.swapaxes(ready_up, 1, 2),
        ready_down,
        scale_gate,
        scale_up,
        scale_down,
        jnp.swapaxes(serve_router, 0, 1),
    )


def solution(mesh):
    in_specs = (
        P("ep", "fsdp", None),
        P("ep", "fsdp", None),
        P("ep", None, "fsdp"),
        P("fsdp", "ep"),
        P("fsdp"),
    )
    out_specs = (
        P("ep", None, "fsdp"),
        P("ep", None, "fsdp"),
        P("ep", "fsdp", None),
        P("ep", "fsdp"),
        P("ep", "fsdp"),
        P("ep", "fsdp"),
        P(),
    )
    return jax.shard_map(shards, mesh=mesh, in_specs=in_specs, out_specs=out_specs, check_vma=False)
```

```python
import jax
import jax.numpy as jnp
from jax import lax
from jax.experimental import pallas as pl
from jax.experimental.pallas import tpu as pltpu
from jax.sharding import PartitionSpec as P

D_MODEL = 2048
SIDE = 4
PEERS = 16
OWN = 8
COLS = 88
LANES = 128
ROWS = OWN * COLS
FIRST_ROWS = 2 * ROWS + OWN
FIRST_LIMIT = 46

HOPS = (
    (1, 1), (3, 3),
    (3, 1), (1, 3),
    (0, 2), (2, 0),
    (2, 2),
    (1, 2), (3, 0),
    (3, 2), (1, 0),
    (2, 1), (0, 3),
    (2, 3), (0, 1),
)
HBM = pl.BlockSpec(memory_space=pltpu.HBM)
ANY = pl.BlockSpec(memory_space=pl.ANY)
VMEM = pl.BlockSpec(memory_space=pltpu.VMEM)
SMEM = pl.BlockSpec(memory_space=pltpu.SMEM)


def moved(me, hop, sign):
    y, x = me // SIDE, me % SIDE
    return (y + SIDE + sign * hop[0]) % SIDE * SIDE + (x + SIDE + sign * hop[1]) % SIDE


def started(copies):
    for copy in copies:
        copy.start()
    return copies


def peers_of(me):
    return [moved(me, hop, 1) for hop in ((0, 0), *HOPS)]


def turned_out(raw, turned, outs, peers, rows):
    whole = raw[...].astype(jnp.bfloat16).T
    for peer in range(PEERS):
        turned[peer] = whole[COLS * peer : COLS * (peer + 1), :]
    for out, peer in zip(outs, peers):
        out[rows, :] = turned[peer]


def cut_out(whole, outs, peers, rows):
    for out, peer in zip(outs, peers):
        part = whole[pl.ds(pl.multiple_of(COLS * peer, 8), COLS), :]
        out[rows, :] = part.astype(jnp.bfloat16)


def pack_first_kernel(me, gate, down, served, *rest):
    outs, (raw_gate, raw_down, turned, sems_gate, sems_down) = rest[:PEERS], rest[PEERS:]
    gates = [pltpu.make_async_copy(gate.at[e], raw_gate.at[e], sems_gate.at[e]) for e in range(OWN)]
    downs = [pltpu.make_async_copy(down.at[e], raw_down.at[e], sems_down.at[e]) for e in range(OWN)]
    for e in range(OWN):
        gates[e].start()
        downs[e].start()
    peers = peers_of(me[0])
    for out in outs:
        out[2 * ROWS :, :] = served[...]
    for e in range(OWN):
        rows = slice(COLS * e, COLS * (e + 1))
        gates[e].wait()
        turned_out(
            raw_gate.at[e], turned.at[e % 2], outs, peers, slice(ROWS + rows.start, ROWS + rows.stop)
        )
        downs[e].wait()
        cut_out(raw_down.at[e], outs, peers, rows)


def pack_first(me, gate, down, served):
    return pl.pallas_call(
        pack_first_kernel,
        in_specs=[SMEM, HBM, HBM, VMEM],
        out_specs=[VMEM] * PEERS,
        out_shape=[jax.ShapeDtypeStruct((FIRST_ROWS, LANES), jnp.bfloat16)] * PEERS,
        scratch_shapes=[
            pltpu.VMEM((OWN, LANES, PEERS * COLS), jnp.float32),
            pltpu.VMEM((OWN, PEERS * COLS, LANES), jnp.float32),
            pltpu.VMEM((2, PEERS, COLS, LANES), jnp.bfloat16),
            pltpu.SemaphoreType.DMA((OWN,)),
            pltpu.SemaphoreType.DMA((OWN,)),
        ],
        compiler_params=pltpu.CompilerParams(vmem_limit_bytes=FIRST_LIMIT << 20),
        name="pack_first",
    )(me, gate, down, served)


def pack_last_kernel(me, up, _, *rest):
    outs, (raw, turned, sems) = rest[:PEERS], rest[PEERS:]
    copies = started([pltpu.make_async_copy(up.at[e], raw.at[e], sems.at[e]) for e in range(OWN)])
    peers = peers_of(me[0])
    for e in range(OWN):
        copies[e].wait()
        turned_out(
            raw.at[e], turned.at[e % 2], outs, peers, slice(COLS * e, COLS * (e + 1))
        )


def pack_last(me, up, after):
    return pl.pallas_call(
        pack_last_kernel,
        in_specs=[SMEM, HBM, ANY],
        out_specs=[VMEM] * PEERS,
        out_shape=[jax.ShapeDtypeStruct((ROWS, LANES), jnp.bfloat16)] * PEERS,
        scratch_shapes=[
            pltpu.VMEM((OWN, LANES, PEERS * COLS), jnp.float32),
            pltpu.VMEM((2, PEERS, COLS, LANES), jnp.bfloat16),
            pltpu.SemaphoreType.DMA((OWN,)),
        ],
        compiler_params=pltpu.CompilerParams(vmem_limit_bytes=10 << 20),
        name="pack_last",
    )(me, up, after)


def factor_of(parts, q, scales):
    rows = slice(COLS * q, COLS * (q + 1))
    total = jnp.abs(parts[0][rows, :].astype(jnp.float32))
    for part in parts[1:]:
        total = total + jnp.abs(part[rows, :].astype(jnp.float32))
    scales[q % OWN : q % OWN + 1, :] = jnp.sum(total.T, axis=0, keepdims=True) / D_MODEL
    return D_MODEL / jnp.sum(total, axis=1, keepdims=True)


def scaled(parts, lanes, made, q, factor):
    rows = slice(COLS * q, COLS * (q + 1))
    for part, here in zip(parts, lanes):
        made[q, :, here] = (part[rows, :].astype(jnp.float32) * factor).astype(jnp.bfloat16)


def finish_kernel(me, parts, outs, routed, made, sems):
    lanes = [
        pl.ds(pl.multiple_of(LANES * moved(me[0], hop, -1), LANES), LANES)
        for hop in ((0, 0), *HOPS)
    ]
    writes = []
    for q in range(len(outs) * OWN):
        ready, scales = outs[q // OWN]
        scaled(parts, lanes, made, q, factor_of(parts, q, scales))
        writes += started([pltpu.make_async_copy(made.at[q], ready.at[q % OWN], sems.at[q])])
    if routed is not None:
        for part, here in zip(parts, lanes):
            routed[:, here] = part[2 * ROWS :, :]
    for copy in writes:
        copy.wait()


def finish_first_kernel(me, *rest):
    parts, (down, scale_down, gate, scale_gate, routed, made, sems) = rest[:PEERS], rest[PEERS:]
    finish_kernel(me, parts, [(down, scale_down), (gate, scale_gate)], routed, made, sems)


def finish_last_kernel(me, gathered, *rest):
    parts, (up, scale_up, served, made, sems, sem) = rest[:PEERS], rest[PEERS:]
    copy = pltpu.make_async_copy(gathered, served, sem)
    copy.start()
    finish_kernel(me, parts, [(up, scale_up)], None, made, sems)
    copy.wait()


READY = jax.ShapeDtypeStruct((OWN, COLS, D_MODEL), jnp.bfloat16)
SCALE = jax.ShapeDtypeStruct((OWN, COLS), jnp.float32)
SERVED = jax.ShapeDtypeStruct((8 * OWN, D_MODEL), jnp.bfloat16)
ROUTED = jax.ShapeDtypeStruct((OWN, D_MODEL), jnp.bfloat16)


def finish_first(me, parts):
    return pl.pallas_call(
        finish_first_kernel,
        in_specs=[SMEM] + [VMEM] * PEERS,
        out_specs=[HBM, VMEM, HBM, VMEM, VMEM],
        out_shape=[READY, SCALE, READY, SCALE, ROUTED],
        scratch_shapes=[
            pltpu.VMEM((2 * OWN, COLS, D_MODEL), jnp.bfloat16),
            pltpu.SemaphoreType.DMA((2 * OWN,)),
        ],
        compiler_params=pltpu.CompilerParams(vmem_limit_bytes=15 << 20),
        name="finish_first",
    )(me, *parts)


def finish_last(me, gathered, parts):
    return pl.pallas_call(
        finish_last_kernel,
        in_specs=[SMEM, ANY] + [VMEM] * PEERS,
        out_specs=[HBM, VMEM, HBM],
        out_shape=[READY, SCALE, SERVED],
        scratch_shapes=[
            pltpu.VMEM((OWN, COLS, D_MODEL), jnp.bfloat16),
            pltpu.SemaphoreType.DMA((OWN,)),
            pltpu.SemaphoreType.DMA,
        ],
        compiler_params=pltpu.CompilerParams(vmem_limit_bytes=9 << 20),
        name="finish_last",
    )(me, gathered, *parts)


def to_owners(parts):
    received = [parts[0]]
    for k, hop in enumerate(HOPS):
        route = [(d, moved(d, hop, 1)) for d in range(PEERS)]
        received.append(lax.ppermute(parts[k + 1], "fsdp", route))
    return received


def shards(train_gate, train_up, train_down, router_weight, router_gain):
    me = lax.axis_index("fsdp").astype(jnp.int32)[None]
    served = (jnp.swapaxes(router_weight, 0, 1) * router_gain[None, :]).astype(jnp.bfloat16)
    first = pack_first(me, train_gate, train_down, served)
    got_first = to_owners(first)
    last = pack_last(me, train_up, first[0])
    got_last = to_owners(last)
    ready_down, scale_down, ready_gate, scale_gate, routed = finish_first(me, got_first)
    gathered = lax.all_gather(routed, "ep", axis=0, tiled=True)
    ready_up, scale_up, serve_router = finish_last(me, gathered, got_last)
    return (
        jnp.swapaxes(ready_gate, 1, 2),
        jnp.swapaxes(ready_up, 1, 2),
        ready_down,
        scale_gate,
        scale_up,
        scale_down,
        jnp.swapaxes(serve_router, 0, 1),
    )


def solution(mesh):
    in_specs = (
        P("ep", "fsdp", None),
        P("ep", "fsdp", None),
        P("ep", None, "fsdp"),
        P("fsdp", "ep"),
        P("fsdp"),
    )
    out_specs = (
        P("ep", None, "fsdp"),
        P("ep", None, "fsdp"),
        P("ep", "fsdp", None),
        P("ep", "fsdp"),
        P("ep", "fsdp"),
        P("ep", "fsdp"),
        P(),
    )
    return jax.shard_map(shards, mesh=mesh, in_specs=in_specs, out_specs=out_specs, check_vma=False)
```

```python
import jax
import jax.numpy as jnp
from jax import lax
from jax.experimental import pallas as pl
from jax.experimental.pallas import tpu as pltpu
from jax.sharding import PartitionSpec as P

D_MODEL = 2048
SIDE = 4
PEERS = 16
OWN = 8
COLS = 88
LANES = 128
ROWS = OWN * COLS
FIRST_ROWS = 2 * ROWS + OWN
FIRST_LIMIT = 46

HOPS = (
    (1, 1), (3, 3),
    (3, 1), (1, 3),
    (0, 2), (2, 0),
    (2, 2),
    (1, 2), (3, 0),
    (3, 2), (1, 0),
    (2, 1), (0, 3),
    (2, 3), (0, 1),
)
HBM = pl.BlockSpec(memory_space=pltpu.HBM)
LATE = (1, 2, 3, 4, 6)
ANY = pl.BlockSpec(memory_space=pl.ANY)
VMEM = pl.BlockSpec(memory_space=pltpu.VMEM)
SMEM = pl.BlockSpec(memory_space=pltpu.SMEM)


def moved(me, hop, sign):
    y, x = me // SIDE, me % SIDE
    return (y + SIDE + sign * hop[0]) % SIDE * SIDE + (x + SIDE + sign * hop[1]) % SIDE


def started(copies):
    for copy in copies:
        copy.start()
    return copies


def peers_of(me):
    return [moved(me, hop, 1) for hop in ((0, 0), *HOPS)]


def turned_out(raw, turned, outs, peers, rows):
    whole = raw[...].astype(jnp.bfloat16).T
    for peer in range(PEERS):
        turned[peer] = whole[COLS * peer : COLS * (peer + 1), :]
    for out, peer in zip(outs, peers):
        out[rows, :] = turned[peer]


def cut_out(whole, outs, peers, rows):
    for out, peer in zip(outs, peers):
        part = whole[pl.ds(pl.multiple_of(COLS * peer, 8), COLS), :]
        out[rows, :] = part.astype(jnp.bfloat16)


def pack_first_kernel(me, gate, down, served, *rest):
    outs, (raw_gate, raw_down, turned, sems_gate, sems_down) = rest[:PEERS], rest[PEERS:]
    gates = [pltpu.make_async_copy(gate.at[e], raw_gate.at[e], sems_gate.at[e]) for e in range(OWN)]
    downs = [pltpu.make_async_copy(down.at[e], raw_down.at[e], sems_down.at[e]) for e in range(OWN)]
    for e in range(OWN):
        gates[e].start()
        downs[e].start()
    peers = peers_of(me[0])
    for out in outs:
        out[2 * ROWS :, :] = served[...]
    for e in range(OWN):
        rows = slice(COLS * e, COLS * (e + 1))
        gates[e].wait()
        turned_out(
            raw_gate.at[e], turned.at[e % 2], outs, peers, slice(ROWS + rows.start, ROWS + rows.stop)
        )
        downs[e].wait()
        cut_out(raw_down.at[e], outs, peers, rows)


def pack_first(me, gate, down, served):
    return pl.pallas_call(
        pack_first_kernel,
        in_specs=[SMEM, HBM, HBM, VMEM],
        out_specs=[VMEM] * PEERS,
        out_shape=[jax.ShapeDtypeStruct((FIRST_ROWS, LANES), jnp.bfloat16)] * PEERS,
        scratch_shapes=[
            pltpu.VMEM((OWN, LANES, PEERS * COLS), jnp.float32),
            pltpu.VMEM((OWN, PEERS * COLS, LANES), jnp.float32),
            pltpu.VMEM((2, PEERS, COLS, LANES), jnp.bfloat16),
            pltpu.SemaphoreType.DMA((OWN,)),
            pltpu.SemaphoreType.DMA((OWN,)),
        ],
        compiler_params=pltpu.CompilerParams(vmem_limit_bytes=FIRST_LIMIT << 20),
        name="pack_first",
    )(me, gate, down, served)


def pack_last_kernel(me, up, _, *rest):
    outs, (raw, turned, sems) = rest[:PEERS], rest[PEERS:]
    copies = started([pltpu.make_async_copy(up.at[e], raw.at[e], sems.at[e]) for e in range(OWN)])
    peers = peers_of(me[0])
    for e in range(OWN):
        copies[e].wait()
        turned_out(
            raw.at[e], turned.at[e % 2], outs, peers, slice(COLS * e, COLS * (e + 1))
        )


def pack_last(me, up, after):
    return pl.pallas_call(
        pack_last_kernel,
        in_specs=[SMEM, HBM, ANY],
        out_specs=[VMEM] * PEERS,
        out_shape=[jax.ShapeDtypeStruct((ROWS, LANES), jnp.bfloat16)] * PEERS,
        scratch_shapes=[
            pltpu.VMEM((OWN, LANES, PEERS * COLS), jnp.float32),
            pltpu.VMEM((2, PEERS, COLS, LANES), jnp.bfloat16),
            pltpu.SemaphoreType.DMA((OWN,)),
        ],
        compiler_params=pltpu.CompilerParams(vmem_limit_bytes=46 << 20),
        name="pack_last",
    )(me, up, after)


def size_of(parts, rows):
    total = jnp.abs(parts[0][rows, :].astype(jnp.float32))
    for part in parts[1:]:
        total = total + jnp.abs(part[rows, :].astype(jnp.float32))
    return total


def factor_of(parts, summed, q, scales):
    rows = slice(COLS * q, COLS * (q + 1))
    if summed is None:
        total = size_of(parts, rows)
    else:
        total = summed[rows, :] + size_of([parts[k] for k in LATE], rows)
    scales[q % OWN : q % OWN + 1, :] = jnp.sum(total.T, axis=0, keepdims=True) / D_MODEL
    return D_MODEL / jnp.sum(total, axis=1, keepdims=True)


def scaled(parts, lanes, made, q, factor):
    rows = slice(COLS * q, COLS * (q + 1))
    for part, here in zip(parts, lanes):
        made[q, :, here] = (part[rows, :].astype(jnp.float32) * factor).astype(jnp.bfloat16)


def finish_kernel(me, parts, summed, outs, routed, made, sems):
    lanes = [
        pl.ds(pl.multiple_of(LANES * moved(me[0], hop, -1), LANES), LANES)
        for hop in ((0, 0), *HOPS)
    ]
    writes = []
    for q in range(len(outs) * OWN):
        ready, scales = outs[q // OWN]
        scaled(parts, lanes, made, q, factor_of(parts, summed, q, scales))
        writes += started([pltpu.make_async_copy(made.at[q], ready.at[q % OWN], sems.at[q])])
    if routed is not None:
        for part, here in zip(parts, lanes):
            routed[:, here] = part[2 * ROWS :, :]
    for copy in writes:
        copy.wait()


def finish_first_kernel(me, *rest):
    parts, (down, scale_down, gate, scale_gate, routed, made, sems) = rest[:PEERS], rest[PEERS:]
    finish_kernel(me, parts, None, [(down, scale_down), (gate, scale_gate)], routed, made, sems)


def finish_last_kernel(me, gathered, summed, *rest):
    parts, (up, scale_up, served, made, sems, sem) = rest[:PEERS], rest[PEERS:]
    copy = pltpu.make_async_copy(gathered, served, sem)
    copy.start()
    finish_kernel(me, parts, summed, [(up, scale_up)], None, made, sems)
    copy.wait()


READY = jax.ShapeDtypeStruct((OWN, COLS, D_MODEL), jnp.bfloat16)
SCALE = jax.ShapeDtypeStruct((OWN, COLS), jnp.float32)
SERVED = jax.ShapeDtypeStruct((8 * OWN, D_MODEL), jnp.bfloat16)
ROUTED = jax.ShapeDtypeStruct((OWN, D_MODEL), jnp.bfloat16)


def finish_first(me, parts):
    return pl.pallas_call(
        finish_first_kernel,
        in_specs=[SMEM] + [VMEM] * PEERS,
        out_specs=[HBM, VMEM, HBM, VMEM, VMEM],
        out_shape=[READY, SCALE, READY, SCALE, ROUTED],
        scratch_shapes=[
            pltpu.VMEM((2 * OWN, COLS, D_MODEL), jnp.bfloat16),
            pltpu.SemaphoreType.DMA((2 * OWN,)),
        ],
        compiler_params=pltpu.CompilerParams(vmem_limit_bytes=15 << 20),
        name="finish_first",
    )(me, *parts)


def presum_kernel(_, *rest):
    parts, summed = rest[:-1], rest[-1]
    for e in range(OWN):
        rows = slice(COLS * e, COLS * (e + 1))
        summed[rows, :] = size_of(parts, rows)


def presum(after, parts):
    early = [part for k, part in enumerate(parts) if k not in LATE]
    return pl.pallas_call(
        presum_kernel,
        in_specs=[ANY] + [VMEM] * len(early),
        out_specs=VMEM,
        out_shape=jax.ShapeDtypeStruct((ROWS, LANES), jnp.float32),
        compiler_params=pltpu.CompilerParams(vmem_limit_bytes=9 << 20),
        name="presum",
    )(after, *early)


def finish_last(me, gathered, summed, parts):
    return pl.pallas_call(
        finish_last_kernel,
        in_specs=[SMEM, ANY, VMEM] + [VMEM] * PEERS,
        out_specs=[HBM, VMEM, HBM],
        out_shape=[READY, SCALE, SERVED],
        scratch_shapes=[
            pltpu.VMEM((OWN, COLS, D_MODEL), jnp.bfloat16),
            pltpu.SemaphoreType.DMA((OWN,)),
            pltpu.SemaphoreType.DMA,
        ],
        compiler_params=pltpu.CompilerParams(vmem_limit_bytes=9 << 20),
        name="finish_last",
    )(me, gathered, summed, *parts)


def to_owners(parts):
    received = [parts[0]]
    for k, hop in enumerate(HOPS):
        route = [(d, moved(d, hop, 1)) for d in range(PEERS)]
        received.append(lax.ppermute(parts[k + 1], "fsdp", route))
    return received


def shards(train_gate, train_up, train_down, router_weight, router_gain):
    me = lax.axis_index("fsdp").astype(jnp.int32)[None]
    served = (jnp.swapaxes(router_weight, 0, 1) * router_gain[None, :]).astype(jnp.bfloat16)
    first = pack_first(me, train_gate, train_down, served)
    got_first = to_owners(first)
    last = pack_last(me, train_up, first[0])
    got_last = to_owners(last)
    ready_down, scale_down, ready_gate, scale_gate, routed = finish_first(me, got_first)
    gathered = lax.all_gather(routed, "ep", axis=0, tiled=True)
    summed = presum(gathered, got_last)
    ready_up, scale_up, serve_router = finish_last(me, gathered, summed, got_last)
    return (
        jnp.swapaxes(ready_gate, 1, 2),
        jnp.swapaxes(ready_up, 1, 2),
        ready_down,
        scale_gate,
        scale_up,
        scale_down,
        jnp.swapaxes(serve_router, 0, 1),
    )


def solution(mesh):
    in_specs = (
        P("ep", "fsdp", None),
        P("ep", "fsdp", None),
        P("ep", None, "fsdp"),
        P("fsdp", "ep"),
        P("fsdp"),
    )
    out_specs = (
        P("ep", None, "fsdp"),
        P("ep", None, "fsdp"),
        P("ep", "fsdp", None),
        P("ep", "fsdp"),
        P("ep", "fsdp"),
        P("ep", "fsdp"),
        P(),
    )
    return jax.shard_map(shards, mesh=mesh, in_specs=in_specs, out_specs=out_specs, check_vma=False)
```
